32 devices in a mesh: seq: 8 (over y, x, core), rep: 4 (over z).
Axes of the slice: x: 2, y: 2, z: 4, core: 2. Of those that a mesh axis runs over, the one named last changes fastest.
Arguments:
- queries: bfloat16 [4096, 2048], P(('rep', 'seq')), parts along dimension 0, may hold values from -6 to 6
- keys: bfloat16 [4096, 2048], P(('rep', 'seq')), parts along dimension 0, may hold values from -6 to 6
- values: bfloat16 [4096, 2048], P(('rep', 'seq')), parts along dimension 0, may hold values from -6 to 6
- short_taps: float32 [3, 3, 2048], replicated, may hold values from -3.5 to 3.5
- decay: float32 [2048, 16], replicated, may hold values from 0.00048828125 to 0.1
- residue: float32 [2048, 16], replicated, may hold values from -1.5 to 1.5
- skip: float32 [2048], replicated, may hold values from -3 to 3
- w_out: bfloat16 [2048, 2048], replicated, may hold values from -0.125 to 0.125
Outputs:
- layer_out: bfloat16 [4096, 2048], P(('rep', 'seq')), parts along dimension 0
The draws below stay inside these ranges and needn't reach their ends.
There are 4 independent parts, one for each index of `rep`. The reference program is written for one: setup_inputs(seed, part) draws one part's arguments, and reference() takes and returns one part's arrays. A program takes and returns all parts, laid end to end along the dimension named above; an argument that names none is the same for every part. Nothing has to cross between parts.
All inputs are finite; a program needn't handle non-finite values.
Results may differ from the reference program's by a relative error of at most 0.014.
Values may be sent and summed in bfloat16 or wider, within the bound.
A program may use at most 64 MiB of HBM per device.

```python
import math
import jax
import jax.numpy as jnp
from jax import lax

D = 2048
MODES = 16
SEQLEN = 1024


def levels(stream_key, extent, shards, smallest, top_value):
    level = 1.0
    for axis_at, parts in shards:
        steps = jax.random.uniform(jax.random.fold_in(jax.random.fold_in(stream_key, 6), axis_at), (parts,), jnp.float32, smallest / len(shards), top_value / len(shards))
        level = level * jnp.repeat(jnp.exp(steps), extent[axis_at] // parts).reshape((-1,) + (1,) * (len(extent) - 1 - axis_at))
    return level


def normal_values(key, extent, deviation, bound, split=(), kind=jnp.bfloat16):
    values = jax.random.normal(key, extent, jnp.float32) * deviation
    if len(split) > 0:
        values = levels(key, extent, split, -0.22, 0.18) * values
    return jnp.clip(values, min=-bound, max=bound).astype(kind)


def setup_inputs(seed: int = 0, part: int = 0) -> dict:
    seeds = jax.random.split(jax.random.key(seed), 9)
    part_keys = jax.random.split(jax.random.fold_in(seeds[8], part), 9)
    return {
        "queries": normal_values(part_keys[0], (SEQLEN, D), 1.0, 6.0, ((0, 8),)),
        "keys": normal_values(part_keys[1], (SEQLEN, D), 1.0, 6.0, ((0, 8),)),
        "values": normal_values(part_keys[2], (SEQLEN, D), 1.0, 6.0, ((0, 8),)),
        "short_taps": normal_values(seeds[3], (3, 3, D), 3 ** -0.5, 3.5, (), jnp.float32),
        "decay": jnp.clip(jnp.exp(jax.random.uniform(seeds[4], (D, MODES), jnp.float32, math.log(0.00048828125), math.log(0.1))), 0.00048828125, 0.1),
        "residue": normal_values(seeds[5], (D, MODES), 0.25, 1.5, (), jnp.float32),
        "skip": normal_values(seeds[6], (D,), 0.5, 3.0, (), jnp.float32),
        "w_out": normal_values(seeds[7], (D, D), D ** -0.5, 0.125),
    }


def short_conv(tokens, taps):
    whole = tokens.astype(jnp.float32)
    width = whole.shape[1]
    result = taps[0] * whole
    first = jnp.concatenate([jnp.zeros((1, width), jnp.float32), whole[:-1]], axis=0)
    second = jnp.concatenate([jnp.zeros((2, width), jnp.float32), whole[:-2]], axis=0)
    return result + taps[1] * first + taps[2] * second

def reference(queries, keys, values, short_taps, decay, residue, skip, w_out):
    q_short = short_conv(queries, short_taps[0])
    k_short = short_conv(keys, short_taps[1])
    v_short = short_conv(values, short_taps[2])
    mixed_in = (k_short * v_short).astype(jnp.bfloat16)
    signal = mixed_in.astype(jnp.float32)
    weights = residue * jnp.sqrt(1.0 - jnp.exp(-2.0 * decay))
    length, width = signal.shape
    group = math.gcd(width, 128)
    count = width // group
    grouped = signal.reshape(length, count, group).transpose(1, 0, 2)
    rate_groups = decay.reshape(count, group, decay.shape[1])
    weight_groups = weights.reshape(count, group, decay.shape[1])

    def one_group(items):
        piece, rates, wts = items
        times = jnp.arange(length, dtype=jnp.float32)
        filt = lax.optimization_barrier(jnp.sum(jnp.exp(-times[:, None, None] * rates[None]) * wts[None], axis=2))
        total = 2 * length
        spectrum = jnp.fft.rfft(piece, total, axis=0) * jnp.fft.rfft(filt, total, axis=0)
        return jnp.fft.irfft(spectrum, total, axis=0)[:length]
    convolved = lax.map(one_group, (grouped, rate_groups, weight_groups))
    convolved = convolved.transpose(1, 0, 2).reshape(length, width)
    long_out = (convolved + skip * signal).astype(jnp.bfloat16)
    gated = (q_short * long_out.astype(jnp.float32)).astype(jnp.bfloat16)
    return jnp.dot(gated, w_out, preferred_element_type=jnp.float32).astype(jnp.bfloat16)
```

```python
import functools
import math

import jax
import jax.numpy as jnp
from jax import lax
from jax.experimental import pallas as pl
from jax.experimental.pallas import tpu as pltpu
from jax.sharding import PartitionSpec as P

MESH = pl.DeviceIdType.MESH
F32 = jnp.float32
SUB = 8


def kernel(
    n, width,
    q_hbm, k_hbm, v_hbm, taps_ref, rates_ref, residue_ref, skip_ref, w_hbm,
    out_ref,
    q_in, k_in, v_in, w_in, tails_out, tails_in, ext, sig, q_short, partial, states,
    carry_table, tap_table, gated, ends, before, totals, earlier, total_out,
    in_sems, w_sem, tail_sems, pair_send, pair_recv, group_send, group_recv,
):
    rows, chans = q_in.shape
    modes = rates_ref.shape[0]
    blocks = rows // SUB
    chunks = chans // width
    groups = n // 2
    me = lax.axis_index("seq")
    group = lax.div(me, 2)
    odd = lax.rem(me, 2)

    barrier = pltpu.get_barrier_semaphore()

    def greet(step, carry):
        pl.semaphore_signal(
            barrier, inc=1, device_id={"seq": lax.rem(me + step, n)}, device_id_type=MESH
        )
        return carry

    lax.fori_loop(1, n, greet, 0)
    loads = [
        pltpu.make_async_copy(src, dst, in_sems.at[i])
        for i, (src, dst) in enumerate(((q_hbm, q_in), (k_hbm, k_in), (v_hbm, v_in)))
    ]
    for load in loads:
        load.start()
    w_load = pltpu.make_async_copy(w_hbm, w_in, w_sem)
    w_load.start()

    for load in loads:
        load.wait()
    for i, tokens in enumerate((q_in, k_in, v_in)):
        last = tokens[rows - 16 :, :].astype(F32)
        tails_out[2 * i : 2 * i + 2, :] = last[14:16]
    tails_out[6:8, :] = jnp.zeros((2, chans), F32)
    pl.semaphore_wait(barrier, n - 1)

    def tail_copy():
        return pltpu.make_async_remote_copy(
            src_ref=tails_out, dst_ref=tails_in, send_sem=tail_sems.at[0], recv_sem=tail_sems.at[1],
            device_id={"seq": lax.rem(me + 1, n)}, device_id_type=MESH,
        )

    def pair_copy(g):
        return pltpu.make_async_remote_copy(
            src_ref=ends.at[g], dst_ref=before.at[g], send_sem=pair_send.at[g], recv_sem=pair_recv.at[g],
            device_id={"seq": me + 1 - 2 * odd}, device_id_type=MESH,
        )

    def group_copy(source, target, core, g):
        return pltpu.make_async_remote_copy(
            src_ref=totals.at[g], dst_ref=earlier.at[source, g],
            send_sem=group_send.at[target, core, g], recv_sem=group_recv.at[source, g],
            device_id={"seq": 2 * target + core}, device_id_type=MESH,
        )

    @pl.when(me < n - 1)
    def _():
        tail_copy().start()

    @pl.when(me == 0)
    def _():
        tails_in[...] = jnp.zeros_like(tails_in)

    @pl.when(odd == 0)
    def _():
        before[...] = jnp.zeros_like(before)

    place = lax.broadcasted_iota(jnp.int32, (SUB, width), 0)
    steps = (place + 1).astype(F32)

    def tables(g, carry):
        cols = pl.ds(pl.multiple_of(g * width, width), width)
        rates = rates_ref[:, cols]
        weights = residue_ref[:, cols] * jnp.sqrt(1.0 - jnp.exp(-2.0 * rates))
        total = jnp.zeros((SUB, width), F32)
        for m in range(modes):
            row = jnp.exp(-rates[m : m + 1] * steps) * weights[m : m + 1]
            carry_table[m * SUB : (m + 1) * SUB, cols] = row
            total = total + row
        first = jnp.sum(weights, axis=0, keepdims=True) + skip_ref[:, cols]
        taps = jnp.where(place == 0, first, pltpu.roll(total, 1, 0))
        for s in range(SUB):
            shifted = taps if s == 0 else jnp.where(place >= s, pltpu.roll(taps, s, 0), 0.0)
            tap_table[s * SUB : (s + 1) * SUB, cols] = shifted
        return carry

    lax.fori_loop(0, chunks, tables, 0)

    @pl.when(me > 0)
    def _():
        tail_copy().wait_recv()

    def combine(g):
        @pl.when(odd == 1)
        def _():
            pair_copy(g).wait_recv()

            @pl.when(group < groups - 1)
            def _():
                cols = pl.ds(pl.multiple_of(g * width, width), width)
                span = jnp.exp(-float(rows) * rates_ref[:, cols])
                totals[g] = span * before[g] + ends[g]

                def send(target, carry):
                    for core in range(2):
                        group_copy(group, target, core, g).start()
                    return carry

                lax.fori_loop(group + 1, groups, send, 0)

    strip = math.gcd(rows, 16)

    def local(g, carry):
        cols = pl.ds(pl.multiple_of(g * width, width), width)
        for i, tokens in enumerate((q_in, k_in, v_in)):
            ext[i, SUB - 2 : SUB, :] = tails_in[2 * i : 2 * i + 2, cols]
            for r in range(0, rows, strip):
                ext[i, SUB + r : SUB + r + strip, :] = tokens[r : r + strip, cols].astype(F32)

        def short(i, r):
            result = taps_ref[i, 0:1, cols] * ext[i, SUB + r : SUB + r + strip, :]
            result = result + taps_ref[i, 1:2, cols] * ext[i, SUB + r - 1 : SUB + r + strip - 1, :]
            return result + taps_ref[i, 2:3, cols] * ext[i, SUB + r - 2 : SUB + r + strip - 2, :]

        for r in range(0, rows, strip):
            mixed = (short(1, r) * short(2, r)).astype(jnp.bfloat16)
            sig[r : r + strip, :] = mixed.astype(F32)
            q_short[r : r + strip, cols] = short(0, r)

        fade = jnp.exp(-rates_ref[:, cols])

        def block(b, state):
            states[pl.ds(pl.multiple_of(b * modes, modes), modes), cols] = state
            base = pl.multiple_of(b * SUB, SUB)
            acc = None
            for s in range(SUB):
                row = sig[pl.ds(base + s, 1), :]
                state = state * fade + row
                term = tap_table[s * SUB : (s + 1) * SUB, cols] * row
                acc = term if acc is None else acc + term
            partial[pl.ds(base, SUB), cols] = acc
            return state

        ends[g] = lax.fori_loop(0, blocks, block, jnp.zeros((modes, width), F32), unroll=2)

        @pl.when(odd == 0)
        def _():
            pair_copy(g).start()

        @pl.when(g > 0)
        def _():
            combine(g - 1)

        return carry

    lax.fori_loop(0, chunks, local, 0)
    combine(chunks - 1)
    w_load.wait()
    batch = 4 if blocks % 4 == 0 else 1
    tile = math.gcd(chans, 512)

    def finish(g, carry):
        cols = pl.ds(pl.multiple_of(g * width, width), width)
        rates = rates_ref[:, cols]
        far = jnp.exp(-2.0 * rows * rates)

        def gather(source, state):
            group_copy(source, group, odd, g).wait_recv()
            return state * far + earlier[source, g]

        entering = lax.fori_loop(0, group, gather, jnp.zeros((modes, width), F32))
        span = jnp.where(odd == 1, jnp.exp(-float(rows) * rates), 1.0)
        entering = span * entering + before[g]
        fade = jnp.exp(-float(SUB) * rates)
        for b in range(blocks):
            here = slice(b * modes, (b + 1) * modes)
            states[here, cols] = states[here, cols] + entering
            entering = entering * fade

        def outputs(k, inner):
            base = pl.multiple_of(k * batch * SUB, batch * SUB)
            accs = [partial[pl.ds(base + j * SUB, SUB), cols] for j in range(batch)]
            for m in range(modes):
                table = carry_table[m * SUB : (m + 1) * SUB, cols]
                for j in range(batch):
                    row = states[pl.ds((k * batch + j) * modes + m, 1), cols]
                    accs[j] = accs[j] + table * row
            long_out = jnp.concatenate(accs, axis=0).astype(jnp.bfloat16).astype(F32)
            here = pl.ds(base, batch * SUB)
            gated[here, :] = (q_short[here, cols] * long_out).astype(jnp.bfloat16)
            return inner

        lax.fori_loop(0, blocks // batch, outputs, 0)
        for c in range(0, chans, tile):
            piece = jnp.dot(gated[...], w_in[cols, c : c + tile], preferred_element_type=F32)
            total_out[:, c : c + tile] += piece
        return carry

    total_out[...] = jnp.zeros_like(total_out)
    lax.fori_loop(0, chunks, finish, 0)
    out_ref[...] = total_out[...].astype(out_ref.dtype)

    @pl.when(me < n - 1)
    def _():
        tail_copy().wait_send()

    @pl.when(odd == 0)
    def _():
        for g in range(chunks):
            pair_copy(g).wait_send()

    @pl.when(odd == 1)
    def _():
        def sent(target, carry):
            for core in range(2):
                for g in range(chunks):
                    group_copy(group, target, core, g).wait_send()
            return carry

        lax.fori_loop(group + 1, groups, sent, 0)


def solution(mesh):
    n = mesh.shape["seq"]

    def body(queries, keys, values, short_taps, decay, residue, skip, w_out):
        rows, chans = queries.shape
        modes = decay.shape[1]
        width = math.gcd(chans, 512)
        chunks = chans // width
        bf16 = jnp.bfloat16
        vmem = pl.BlockSpec(memory_space=pltpu.VMEM)
        hbm = pl.BlockSpec(memory_space=pl.ANY)
        dma = pltpu.SemaphoreType.DMA
        return pl.pallas_call(
            functools.partial(kernel, n, width),
            out_shape=jax.ShapeDtypeStruct((rows, w_out.shape[1]), bf16),
            in_specs=[hbm, hbm, hbm, vmem, vmem, vmem, vmem, hbm],
            out_specs=vmem,
            scratch_shapes=[
                pltpu.VMEM((rows, chans), bf16),
                pltpu.VMEM((rows, chans), bf16),
                pltpu.VMEM((rows, chans), bf16),
                pltpu.VMEM(w_out.shape, bf16),
                pltpu.VMEM((SUB, chans), F32),
                pltpu.VMEM((SUB, chans), F32),
                pltpu.VMEM((3, rows + SUB, width), F32),
                pltpu.VMEM((rows, width), F32),
                pltpu.VMEM((rows, chans), F32),
                pltpu.VMEM((rows, chans), F32),
                pltpu.VMEM((rows // SUB * modes, chans), F32),
                pltpu.VMEM((modes * SUB, chans), F32),
                pltpu.VMEM((SUB * SUB, chans), F32),
                pltpu.VMEM((rows, width), bf16),
                pltpu.VMEM((chunks, modes, width), F32),
                pltpu.VMEM((chunks, modes, width), F32),
                pltpu.VMEM((chunks, modes, width), F32),
                pltpu.VMEM((n // 2, chunks, modes, width), F32),
                pltpu.VMEM((rows, w_out.shape[1]), F32),
                dma((3,)),
                dma,
                dma((2,)),
                dma((chunks,)),
                dma((chunks,)),
                dma((n // 2, 2, chunks)),
                dma((n // 2, chunks)),
            ],
            compiler_params=pltpu.CompilerParams(
                collective_id=0, has_side_effects=True, vmem_limit_bytes=60 * 1024 * 1024
            ),
        )(queries, keys, values, short_taps, decay.T, residue.T, skip[None, :], w_out)

    placed = (P(("rep", "seq"), None),) * 3 + (P(),) * 5
    return jax.shard_map(
        body, mesh=mesh, in_specs=placed, out_specs=P(("rep", "seq"), None), check_vma=False
    )
```

```python
import functools
import math

import jax
import jax.numpy as jnp
from jax import lax
from jax.experimental import pallas as pl
from jax.experimental.pallas import tpu as pltpu
from jax.sharding import PartitionSpec as P

MESH = pl.DeviceIdType.MESH
F32 = jnp.float32
SUB = 8


def kernel(
    n, width,
    q_hbm, k_hbm, v_hbm, taps_hbm, rates_hbm, residue_hbm, skip_hbm, w_hbm,
    out_ref,
    q_in, k_in, v_in, taps_ref, rates_ref, residue_ref, skip_ref, w_in, tails_out, tails_in, ext, sig, q_short, partial, states,
    carry_table, tap_table, gated, ends, before, totals, earlier, total_out,
    in_sems, w_sem, tail_sems, pair_send, pair_recv, group_send, group_recv,
):
    rows, chans = q_in.shape
    modes = rates_ref.shape[0]
    blocks = rows // SUB
    chunks = chans // width
    groups = n // 2
    me = lax.axis_index("seq")
    group = lax.div(me, 2)
    odd = lax.rem(me, 2)

    barrier = pltpu.get_barrier_semaphore()

    def greet(step, carry):
        pl.semaphore_signal(
            barrier, inc=1, device_id={"seq": lax.rem(me + step, n)}, device_id_type=MESH
        )
        return carry

    lax.fori_loop(1, n, greet, 0)
    loads = [
        pltpu.make_async_copy(src, dst, in_sems.at[i])
        for i, (src, dst) in enumerate((
            (q_hbm, q_in), (k_hbm, k_in), (v_hbm, v_in), (rates_hbm, rates_ref),
            (residue_hbm, residue_ref), (skip_hbm, skip_ref), (taps_hbm, taps_ref),
        ))
    ]
    for load in loads:
        load.start()
    w_load = pltpu.make_async_copy(w_hbm, w_in, w_sem)
    w_load.start()

    for load in loads[:3]:
        load.wait()
    for i, tokens in enumerate((q_in, k_in, v_in)):
        last = tokens[rows - 16 :, :].astype(F32)
        tails_out[2 * i : 2 * i + 2, :] = last[14:16]
    tails_out[6:8, :] = jnp.zeros((2, chans), F32)
    pl.semaphore_wait(barrier, n - 1)

    def tail_copy():
        return pltpu.make_async_remote_copy(
            src_ref=tails_out, dst_ref=tails_in, send_sem=tail_sems.at[0], recv_sem=tail_sems.at[1],
            device_id={"seq": lax.rem(me + 1, n)}, device_id_type=MESH,
        )

    def pair_copy(g):
        return pltpu.make_async_remote_copy(
            src_ref=ends.at[g], dst_ref=before.at[g], send_sem=pair_send.at[g], recv_sem=pair_recv.at[g],
            device_id={"seq": me + 1 - 2 * odd}, device_id_type=MESH,
        )

    def group_copy(source, target, core, g):
        return pltpu.make_async_remote_copy(
            src_ref=totals.at[g], dst_ref=earlier.at[source, g],
            send_sem=group_send.at[target, core, g], recv_sem=group_recv.at[source, g],
            device_id={"seq": 2 * target + core}, device_id_type=MESH,
        )

    @pl.when(me < n - 1)
    def _():
        tail_copy().start()

    @pl.when(me == 0)
    def _():
        tails_in[...] = jnp.zeros_like(tails_in)

    @pl.when(odd == 0)
    def _():
        before[...] = jnp.zeros_like(before)

    for load in loads[3:]:
        load.wait()

    place = lax.broadcasted_iota(jnp.int32, (SUB, width), 0)
    steps = (place + 1).astype(F32)

    def tables(g, carry):
        cols = pl.ds(pl.multiple_of(g * width, width), width)
        rates = rates_ref[:, cols]
        weights = residue_ref[:, cols] * jnp.sqrt(1.0 - jnp.exp(-2.0 * rates))
        total = jnp.zeros((SUB, width), F32)
        for m in range(modes):
            row = jnp.exp(-rates[m : m + 1] * steps) * weights[m : m + 1]
            carry_table[m * SUB : (m + 1) * SUB, cols] = row
            total = total + row
        first = jnp.sum(weights, axis=0, keepdims=True) + skip_ref[:, cols]
        taps = jnp.where(place == 0, first, pltpu.roll(total, 1, 0))
        for s in range(SUB):
            shifted = taps if s == 0 else jnp.where(place >= s, pltpu.roll(taps, s, 0), 0.0)
            tap_table[s * SUB : (s + 1) * SUB, cols] = shifted
        return carry

    lax.fori_loop(0, chunks, tables, 0)

    strip = math.gcd(rows, 16)

    def mix(g, first, last):
        cols = pl.ds(pl.multiple_of(g * width, width), width)
        for i, tokens in enumerate((q_in, k_in, v_in)):
            for r in range(max(first - strip, 0), last, strip):
                ext[i, SUB + r : SUB + r + strip, :] = tokens[r : r + strip, cols].astype(F32)

        def short(i, r):
            result = taps_ref[i, 0:1, cols] * ext[i, SUB + r : SUB + r + strip, :]
            result = result + taps_ref[i, 1:2, cols] * ext[i, SUB + r - 1 : SUB + r + strip - 1, :]
            return result + taps_ref[i, 2:3, cols] * ext[i, SUB + r - 2 : SUB + r + strip - 2, :]

        for r in range(first, last, strip):
            mixed = (short(1, r) * short(2, r)).astype(jnp.bfloat16)
            mixed = mixed.astype(F32)
            for j in range(0, strip, SUB):
                sig[(r + j) // SUB, :, cols] = mixed[j : j + SUB]
            q_short[r : r + strip, cols] = short(0, r)

    def mix_later(g, carry):
        mix(g, strip, rows)
        return carry

    lax.fori_loop(0, chunks, mix_later, 0)

    @pl.when(me > 0)
    def _():
        tail_copy().wait_recv()

    def combine(g):
        @pl.when(odd == 1)
        def _():
            pair_copy(g).wait_recv()

            @pl.when(group < groups - 1)
            def _():
                cols = pl.ds(pl.multiple_of(g * width, width), width)
                span = jnp.exp(-float(rows) * rates_ref[:, cols])
                totals[g] = (span * before[g] + ends[g]).astype(totals.dtype)

                def send(target, carry):
                    for core in range(2):
                        group_copy(group, target, core, g).start()
                    return carry

                lax.fori_loop(group + 1, groups, send, 0)

    def local(g, carry):
        cols = pl.ds(pl.multiple_of(g * width, width), width)
        for i in range(3):
            ext[i, SUB - 2 : SUB, :] = tails_in[2 * i : 2 * i + 2, cols]
        mix(g, 0, strip)
        fade = jnp.exp(-rates_ref[:, cols])

        def block(b, state):
            states[b, :, cols] = state
            base = pl.multiple_of(b * SUB, SUB)
            acc = None
            for s in range(SUB):
                row = sig[b, s : s + 1, cols]
                state = state * fade + row
                term = tap_table[s * SUB : (s + 1) * SUB, cols] * row
                acc = term if acc is None else acc + term
            partial[pl.ds(base, SUB), cols] = acc
            return state

        ends[g] = lax.fori_loop(0, blocks, block, jnp.zeros((modes, width), F32), unroll=2)

        @pl.when(odd == 0)
        def _():
            pair_copy(g).start()

        @pl.when(g > 0)
        def _():
            combine(g - 1)

        return carry

    lax.fori_loop(0, chunks, local, 0)
    combine(chunks - 1)
    w_load.wait()
    batch = 4 if blocks % 4 == 0 else 1
    tile = out_ref.shape[1] // (blocks // batch)

    def project(g, side, k):
        source = pl.ds(pl.multiple_of(g * width, width), width)
        here = pl.ds(pl.multiple_of(k * tile, tile), tile)
        piece = jnp.dot(gated[side], w_in[source, here], preferred_element_type=F32)
        total_out[:, here] += piece

    def finish(g, carry):
        cols = pl.ds(pl.multiple_of(g * width, width), width)
        rates = rates_ref[:, cols]
        far = jnp.exp(-2.0 * rows * rates)

        def gather(source, state):
            group_copy(source, group, odd, g).wait_recv()
            return state * far + earlier[source, g].astype(F32)

        entering = lax.fori_loop(0, group, gather, jnp.zeros((modes, width), F32))
        span = jnp.where(odd == 1, jnp.exp(-float(rows) * rates), 1.0)
        entering = span * entering + before[g]
        fade = jnp.exp(-float(SUB) * rates)
        for b in range(blocks):
            states[b, :, cols] = states[b, :, cols] + entering
            entering = entering * fade

        side = lax.rem(g, 2)

        def outputs(k, inner):
            project(jnp.maximum(g - 1, 0), 1 - side, k)
            base = pl.multiple_of(k * batch * SUB, batch * SUB)
            accs = [partial[pl.ds(base + j * SUB, SUB), cols] for j in range(batch)]
            for m in range(modes):
                table = carry_table[m * SUB : (m + 1) * SUB, cols]
                for j in range(batch):
                    row = states[k * batch + j, m : m + 1, cols]
                    accs[j] = accs[j] + table * row
            long_out = jnp.concatenate(accs, axis=0).astype(jnp.bfloat16).astype(F32)
            here = pl.ds(base, batch * SUB)
            gated[side, here, :] = (q_short[here, cols] * long_out).astype(jnp.bfloat16)
            return inner

        lax.fori_loop(0, blocks // batch, outputs, 0)
        return carry

    gated[1] = jnp.zeros(gated.shape[1:], gated.dtype)
    total_out[...] = jnp.zeros_like(total_out)
    lax.fori_loop(0, chunks, finish, 0)
    for k in range(blocks // batch):
        here = slice(k * tile, (k + 1) * tile)
        piece = jnp.dot(
            gated[(chunks - 1) % 2], w_in[chans - width :, here], preferred_element_type=F32
        )
        out_ref[:, here] = (total_out[:, here] + piece).astype(out_ref.dtype)

    @pl.when(me < n - 1)
    def _():
        tail_copy().wait_send()

    @pl.when(odd == 0)
    def _():
        for g in range(chunks):
            pair_copy(g).wait_send()

    @pl.when(odd == 1)
    def _():
        def sent(target, carry):
            for core in range(2):
                for g in range(chunks):
                    group_copy(group, target, core, g).wait_send()
            return carry

        lax.fori_loop(group + 1, groups, sent, 0)


def solution(mesh):
    n = mesh.shape["seq"]

    def body(queries, keys, values, short_taps, decay, residue, skip, w_out):
        rows, chans = queries.shape
        modes = decay.shape[1]
        width = math.gcd(chans, 512)
        chunks = chans // width
        bf16 = jnp.bfloat16
        vmem = pl.BlockSpec(memory_space=pltpu.VMEM)
        hbm = pl.BlockSpec(memory_space=pl.ANY)
        dma = pltpu.SemaphoreType.DMA
        return pl.pallas_call(
            functools.partial(kernel, n, width),
            out_shape=jax.ShapeDtypeStruct((rows, w_out.shape[1]), bf16),
            in_specs=[hbm] * 8,
            out_specs=vmem,
            scratch_shapes=[
                pltpu.VMEM((rows, chans), bf16),
                pltpu.VMEM((rows, chans), bf16),
                pltpu.VMEM((rows, chans), bf16),
                pltpu.VMEM(short_taps.shape, F32),
                pltpu.VMEM((modes, chans), F32),
                pltpu.VMEM((modes, chans), F32),
                pltpu.VMEM((1, chans), F32),
                pltpu.VMEM(w_out.shape, bf16),
                pltpu.VMEM((SUB, chans), F32),
                pltpu.VMEM((SUB, chans), F32),
                pltpu.VMEM((3, rows + SUB, width), F32),
                pltpu.VMEM((rows // SUB, SUB, chans), F32),
                pltpu.VMEM((rows, chans), F32),
                pltpu.VMEM((rows, chans), F32),
                pltpu.VMEM((rows // SUB, modes, chans), F32),
                pltpu.VMEM((modes * SUB, chans), F32),
                pltpu.VMEM((SUB * SUB, chans), F32),
                pltpu.VMEM((2, rows, width), bf16),
                pltpu.VMEM((chunks, modes, width), F32),
                pltpu.VMEM((chunks, modes, width), F32),
                pltpu.VMEM((chunks, modes, width), bf16),
                pltpu.VMEM((n // 2, chunks, modes, width), bf16),
                pltpu.VMEM((rows, w_out.shape[1]), F32),
                dma((7,)),
                dma,
                dma((2,)),
                dma((chunks,)),
                dma((chunks,)),
                dma((n // 2, 2, chunks)),
                dma((n // 2, chunks)),
            ],
            compiler_params=pltpu.CompilerParams(
                collective_id=0, has_side_effects=True, vmem_limit_bytes=60 * 1024 * 1024
            ),
        )(queries, keys, values, short_taps, decay.T, residue.T, skip[None, :], w_out)

    placed = (P(("rep", "seq"), None),) * 3 + (P(),) * 5
    return jax.shard_map(
        body, mesh=mesh, in_specs=placed, out_specs=P(("rep", "seq"), None), check_vma=False
    )
```

```python
import functools
import math

import jax
import jax.numpy as jnp
from jax import lax
from jax.experimental import pallas as pl
from jax.experimental.pallas import tpu as pltpu
from jax.sharding import PartitionSpec as P

MESH = pl.DeviceIdType.MESH
F32 = jnp.float32
SUB = 8


def kernel(
    n, width,
    q_hbm, k_hbm, v_hbm, taps_hbm, rates_hbm, residue_hbm, skip_hbm, w_hbm,
    out_ref,
    q_in, k_in, v_in, taps_ref, rates_ref, residue_ref, skip_ref, w_in, tails_out, tails_in, ext, sig, q_short, partial, states,
    carry_table, tap_table, gated, ends, before, totals, earlier, total_out,
    in_sems, w_sem, tail_sems, pair_send, pair_recv, group_send, group_recv,
):
    rows, chans = q_in.shape
    modes = rates_ref.shape[0]
    blocks = rows // SUB
    chunks = chans // width
    groups = n // 2
    me = lax.axis_index("seq")
    group = lax.div(me, 2)
    odd = lax.rem(me, 2)

    barrier = pltpu.get_barrier_semaphore()

    def greet(step, carry):
        pl.semaphore_signal(
            barrier, inc=1, device_id={"seq": lax.rem(me + step, n)}, device_id_type=MESH
        )
        return carry

    lax.fori_loop(1, n, greet, 0)
    loads = [
        pltpu.make_async_copy(src, dst, in_sems.at[i])
        for i, (src, dst) in enumerate((
            (q_hbm, q_in), (k_hbm, k_in), (v_hbm, v_in), (rates_hbm, rates_ref),
            (residue_hbm, residue_ref), (skip_hbm, skip_ref), (taps_hbm, taps_ref),
        ))
    ]
    for load in loads:
        load.start()
    w_load = pltpu.make_async_copy(w_hbm, w_in, w_sem)

    for load in loads[:3]:
        load.wait()
    w_load.start()
    for i, tokens in enumerate((q_in, k_in, v_in)):
        last = tokens[rows - 16 :, :].astype(F32)
        tails_out[2 * i : 2 * i + 2, :] = last[14:16]
    tails_out[6:8, :] = jnp.zeros((2, chans), F32)
    pl.semaphore_wait(barrier, n - 1)

    def tail_copy():
        return pltpu.make_async_remote_copy(
            src_ref=tails_out, dst_ref=tails_in, send_sem=tail_sems.at[0], recv_sem=tail_sems.at[1],
            device_id={"seq": lax.rem(me + 1, n)}, device_id_type=MESH,
        )

    def pair_copy(g):
        return pltpu.make_async_remote_copy(
            src_ref=ends.at[g], dst_ref=before.at[g], send_sem=pair_send.at[g], recv_sem=pair_recv.at[g],
            device_id={"seq": me + 1 - 2 * odd}, device_id_type=MESH,
        )

    def group_copy(source, target, core, g):
        return pltpu.make_async_remote_copy(
            src_ref=totals.at[g], dst_ref=earlier.at[source, g],
            send_sem=group_send.at[target, core, g], recv_sem=group_recv.at[source, g],
            device_id={"seq": 2 * target + core}, device_id_type=MESH,
        )

    @pl.when(me < n - 1)
    def _():
        tail_copy().start()

    @pl.when(me == 0)
    def _():
        tails_in[...] = jnp.zeros_like(tails_in)

    @pl.when(odd == 0)
    def _():
        before[...] = jnp.zeros_like(before)

    for load in loads[3:]:
        load.wait()

    place = lax.broadcasted_iota(jnp.int32, (SUB, width), 0)
    steps = (place + 1).astype(F32)

    def tables(g, carry):
        cols = pl.ds(pl.multiple_of(g * width, width), width)
        rates = rates_ref[:, cols]
        weights = residue_ref[:, cols] * jnp.sqrt(1.0 - jnp.exp(-2.0 * rates))
        total = jnp.zeros((SUB, width), F32)
        for m in range(modes):
            row = jnp.exp(-rates[m : m + 1] * steps) * weights[m : m + 1]
            carry_table[m * SUB : (m + 1) * SUB, cols] = row
            total = total + row
        first = jnp.sum(weights, axis=0, keepdims=True) + skip_ref[:, cols]
        taps = jnp.where(place == 0, first, pltpu.roll(total, 1, 0))
        for s in range(SUB):
            shifted = taps if s == 0 else jnp.where(place >= s, pltpu.roll(taps, s, 0), 0.0)
            tap_table[s * SUB : (s + 1) * SUB, cols] = shifted
        return carry

    lax.fori_loop(0, chunks, tables, 0)

    strip = math.gcd(rows, 16)

    def mix(g, first, last):
        cols = pl.ds(pl.multiple_of(g * width, width), width)
        for i, tokens in enumerate((q_in, k_in, v_in)):
            for r in range(max(first - strip, 0), last, strip):
                ext[i, SUB + r : SUB + r + strip, :] = tokens[r : r + strip, cols].astype(F32)

        def short(i, r):
            result = taps_ref[i, 0:1, cols] * ext[i, SUB + r : SUB + r + strip, :]
            result = result + taps_ref[i, 1:2, cols] * ext[i, SUB + r - 1 : SUB + r + strip - 1, :]
            return result + taps_ref[i, 2:3, cols] * ext[i, SUB + r - 2 : SUB + r + strip - 2, :]

        for r in range(first, last, strip):
            mixed = (short(1, r) * short(2, r)).astype(jnp.bfloat16)
            mixed = mixed.astype(F32)
            for j in range(0, strip, SUB):
                sig[(r + j) // SUB, :, cols] = mixed[j : j + SUB]
            q_short[r : r + strip, cols] = short(0, r)

    def mix_later(g, carry):
        mix(g, strip, rows)
        return carry

    lax.fori_loop(0, chunks, mix_later, 0)

    @pl.when(me > 0)
    def _():
        tail_copy().wait_recv()

    def combine(g):
        @pl.when(odd == 1)
        def _():
            pair_copy(g).wait_recv()

            @pl.when(group < groups - 1)
            def _():
                cols = pl.ds(pl.multiple_of(g * width, width), width)
                span = jnp.exp(-float(rows) * rates_ref[:, cols])
                totals[g] = (span * before[g] + ends[g]).astype(totals.dtype)

                def send(target, carry):
                    for core in range(2):
                        group_copy(group, target, core, g).start()
                    return carry

                lax.fori_loop(group + 1, groups, send, 0)

    def local(g, carry):
        cols = pl.ds(pl.multiple_of(g * width, width), width)
        for i in range(3):
            ext[i, SUB - 2 : SUB, :] = tails_in[2 * i : 2 * i + 2, cols]
        mix(g, 0, strip)
        fade = jnp.exp(-rates_ref[:, cols])

        def block(b, state):
            states[b, :, cols] = state
            base = pl.multiple_of(b * SUB, SUB)
            acc = None
            for s in range(SUB):
                row = sig[b, s : s + 1, cols]
                state = state * fade + row
                term = tap_table[s * SUB : (s + 1) * SUB, cols] * row
                acc = term if acc is None else acc + term
            partial[pl.ds(base, SUB), cols] = acc
            return state

        ends[g] = lax.fori_loop(0, blocks, block, jnp.zeros((modes, width), F32), unroll=2)

        @pl.when(odd == 0)
        def _():
            pair_copy(g).start()

        @pl.when(g > 0)
        def _():
            combine(g - 1)

        return carry

    lax.fori_loop(0, chunks, local, 0)
    combine(chunks - 1)
    w_load.wait()
    batch = 4 if blocks % 4 == 0 else 1
    tile = out_ref.shape[1] // (blocks // batch)

    def project(g, side, k):
        source = pl.ds(pl.multiple_of(g * width, width), width)
        here = pl.ds(pl.multiple_of(k * tile, tile), tile)
        piece = jnp.dot(gated[side], w_in[source, here], preferred_element_type=F32)
        total_out[:, here] += piece

    def finish(g, carry):
        cols = pl.ds(pl.multiple_of(g * width, width), width)
        rates = rates_ref[:, cols]
        far = jnp.exp(-2.0 * rows * rates)

        def gather(source, state):
            group_copy(source, group, odd, g).wait_recv()
            return state * far + earlier[source, g].astype(F32)

        entering = lax.fori_loop(0, group, gather, jnp.zeros((modes, width), F32))
        span = jnp.where(odd == 1, jnp.exp(-float(rows) * rates), 1.0)
        entering = span * entering + before[g]
        fade = jnp.exp(-float(SUB) * rates)
        for b in range(blocks):
            states[b, :, cols] = states[b, :, cols] + entering
            entering = entering * fade

        side = lax.rem(g, 2)

        def outputs(k, inner):
            project(jnp.maximum(g - 1, 0), 1 - side, k)
            base = pl.multiple_of(k * batch * SUB, batch * SUB)
            accs = [partial[pl.ds(base + j * SUB, SUB), cols] for j in range(batch)]
            for m in range(modes):
                table = carry_table[m * SUB : (m + 1) * SUB, cols]
                for j in range(batch):
                    row = states[k * batch + j, m : m + 1, cols]
                    accs[j] = accs[j] + table * row
            long_out = jnp.concatenate(accs, axis=0).astype(jnp.bfloat16).astype(F32)
            here = pl.ds(base, batch * SUB)
            gated[side, here, :] = (q_short[here, cols] * long_out).astype(jnp.bfloat16)
            return inner

        lax.fori_loop(0, blocks // batch, outputs, 0)
        return carry

    gated[1] = jnp.zeros(gated.shape[1:], gated.dtype)
    total_out[...] = jnp.zeros_like(total_out)
    lax.fori_loop(0, chunks, finish, 0)
    for k in range(blocks // batch):
        here = slice(k * tile, (k + 1) * tile)
        piece = jnp.dot(
            gated[(chunks - 1) % 2], w_in[chans - width :, here], preferred_element_type=F32
        )
        out_ref[:, here] = (total_out[:, here] + piece).astype(out_ref.dtype)

    @pl.when(me < n - 1)
    def _():
        tail_copy().wait_send()

    @pl.when(odd == 0)
    def _():
        for g in range(chunks):
            pair_copy(g).wait_send()

    @pl.when(odd == 1)
    def _():
        def sent(target, carry):
            for core in range(2):
                for g in range(chunks):
                    group_copy(group, target, core, g).wait_send()
            return carry

        lax.fori_loop(group + 1, groups, sent, 0)


def solution(mesh):
    n = mesh.shape["seq"]

    def body(queries, keys, values, short_taps, decay, residue, skip, w_out):
        rows, chans = queries.shape
        modes = decay.shape[1]
        width = math.gcd(chans, 512)
        chunks = chans // width
        bf16 = jnp.bfloat16
        vmem = pl.BlockSpec(memory_space=pltpu.VMEM)
        hbm = pl.BlockSpec(memory_space=pl.ANY)
        dma = pltpu.SemaphoreType.DMA
        return pl.pallas_call(
            functools.partial(kernel, n, width),
            out_shape=jax.ShapeDtypeStruct((rows, w_out.shape[1]), bf16),
            in_specs=[hbm] * 8,
            out_specs=vmem,
            scratch_shapes=[
                pltpu.VMEM((rows, chans), bf16),
                pltpu.VMEM((rows, chans), bf16),
                pltpu.VMEM((rows, chans), bf16),
                pltpu.VMEM(short_taps.shape, F32),
                pltpu.VMEM((modes, chans), F32),
                pltpu.VMEM((modes, chans), F32),
                pltpu.VMEM((1, chans), F32),
                pltpu.VMEM(w_out.shape, bf16),
                pltpu.VMEM((SUB, chans), F32),
                pltpu.VMEM((SUB, chans), F32),
                pltpu.VMEM((3, rows + SUB, width), F32),
                pltpu.VMEM((rows // SUB, SUB, chans), F32),
                pltpu.VMEM((rows, chans), F32),
                pltpu.VMEM((rows, chans), F32),
                pltpu.VMEM((rows // SUB, modes, chans), F32),
                pltpu.VMEM((modes * SUB, chans), F32),
                pltpu.VMEM((SUB * SUB, chans), F32),
                pltpu.VMEM((2, rows, width), bf16),
                pltpu.VMEM((chunks, modes, width), F32),
                pltpu.VMEM((chunks, modes, width), F32),
                pltpu.VMEM((chunks, modes, width), bf16),
                pltpu.VMEM((n // 2, chunks, modes, width), bf16),
                pltpu.VMEM((rows, w_out.shape[1]), F32),
                dma((7,)),
                dma,
                dma((2,)),
                dma((chunks,)),
                dma((chunks,)),
                dma((n // 2, 2, chunks)),
                dma((n // 2, chunks)),
            ],
            compiler_params=pltpu.CompilerParams(
                collective_id=0, has_side_effects=True, vmem_limit_bytes=54272 * 1024
            ),
        )(queries, keys, values, short_taps, decay.T, residue.T, skip[None, :], w_out)

    placed = (P(("rep", "seq"), None),) * 3 + (P(),) * 5
    return jax.shard_map(
        body, mesh=mesh, in_specs=placed, out_specs=P(("rep", "seq"), None), check_vma=False
    )
```
